32 devices in a mesh: ep: 4 (over y, x), fsdp: 8 (over z, core).
Axes of the slice: x: 2, y: 2, z: 4, core: 2. Of those that a mesh axis runs over, the one named last changes fastest.
Arguments:
- train_gate: float32 [64, 2048, 1408], P('ep', 'fsdp'), may hold values from -0.1875 to 0.1875
- other_gate: bfloat16 [64, 2048, 1408], P('ep', 'fsdp'), may hold values from -0.0625 to 0.0625
- train_up: float32 [64, 2048, 1408], P('ep', 'fsdp'), may hold values from -0.1875 to 0.1875
- other_up: bfloat16 [64, 2048, 1408], P('ep', 'fsdp'), may hold values from -0.0625 to 0.0625
- router_weight: float32 [2048, 64], P('fsdp', 'ep'), may hold values from -0.125 to 0.125
- router_gain: float32 [2048], P('fsdp'), may hold values from 0.25 to 1.75
Outputs:
- ready_gate: bfloat16 [64, 2048, 1408], P('ep', None, 'fsdp')
- ready_up: bfloat16 [64, 2048, 1408], P('ep', None, 'fsdp')
- scale_gate: float32 [64, 1408], P('ep', 'fsdp')
- scale_up: float32 [64, 1408], P('ep', 'fsdp')
- serve_router: bfloat16 [2048, 64], replicated
The draws below stay inside these ranges and needn't reach their ends.
All inputs are finite; a program needn't handle non-finite values. Where the reference program divides by a largest or mean magnitude, that divisor is 1e-20 or more.
Results may differ from the reference program's by a relative error of at most 0.001.
Values may be sent and summed in bfloat16 or wider, within the bound.
No kernel may reach another device: no remote copies, remote signals or barrier semaphores. Data moves between devices by JAX's collectives and lax.ppermute only.
A program may use at most 192 MiB of HBM per device.

```python
import jax
import jax.numpy as jnp

EXPERTS = 64
D_MODEL = 2048
D_EXPERT = 1408


def strengthened(array, stream_key, source, target, blocks, factor):
    owner, partner = [(jnp.arange(array.shape[axis_at]) // (array.shape[axis_at] // blocks)).reshape([-1 if axis == axis_at else 1 for axis in range(array.ndim)]) for axis_at in (source, target)]
    chosen = jax.random.permutation(stream_key, blocks)[partner]
    strong = (owner == chosen) | (owner == (partner + blocks // 2) % blocks)
    return jnp.where(strong, factor * array, array)


def steps_of(rng, shape, split, smallest, high):
    def one(axis_at, shards_of):
        heights = jax.random.uniform(jax.random.fold_in(jax.random.fold_in(rng, 6), axis_at), (shards_of,), jnp.float32, smallest / len(split), high / len(split))
        return jnp.repeat(jnp.exp(heights), shape[axis_at] // shards_of).reshape((-1,) + (1,) * (len(shape) - axis_at - 1))

    factor_of = one(*split[0])
    for cut in split[1:]:
        factor_of = factor_of * one(*cut)
    return factor_of


def normal_values(own_key, extent, spread, limit, cuts=(), held_as=jnp.bfloat16):
    entries = spread * jax.random.normal(own_key, extent, jnp.float32)
    if cuts:
        entries = entries * steps_of(own_key, extent, cuts, -0.22, 0.18)
    return jnp.clip(entries, -limit, limit).astype(held_as)


def bell_draw_with(stream_key, shape, spread, most, split, heavy, dtype=jnp.bfloat16):
    result = spread * jax.random.normal(stream_key, shape, jnp.float32)
    if split:
        result = result * steps_of(stream_key, shape, split, -0.22, 0.18)
    return jnp.clip(strengthened(result, jax.random.fold_in(stream_key, 3), *heavy), -most, most).astype(dtype)


def setup_inputs(seed: int = 0) -> dict:
    splits = jax.random.split(jax.random.key(seed), 7)
    train_gate = bell_draw_with(splits[0], (EXPERTS, D_MODEL, D_EXPERT), D_MODEL ** -0.5, 0.1875, ((0, 4), (1, 8)), (1, 2, 8, 2.0), jnp.float32)
    other_gate = normal_values(splits[1], (EXPERTS, D_MODEL, D_EXPERT), (D_MODEL * 4) ** -0.5, 0.0625, ((0, 4), (1, 8)))
    train_up = bell_draw_with(splits[2], (EXPERTS, D_MODEL, D_EXPERT), D_MODEL ** -0.5, 0.1875, ((0, 4), (1, 8)), (1, 2, 8, 2.0), jnp.float32)
    other_up = normal_values(splits[3], (EXPERTS, D_MODEL, D_EXPERT), (D_MODEL * 4) ** -0.5, 0.0625, ((0, 4), (1, 8)))
    router_weight = normal_values(splits[4], (D_MODEL, EXPERTS), D_MODEL ** -0.5, 0.125, ((0, 8), (1, 4)), jnp.float32)
    router_gain = jnp.clip(1.0 + 0.15 * jax.random.normal(splits[5], (D_MODEL,), jnp.float32), 0.25, 1.75)
    return dict(train_gate=train_gate, other_gate=other_gate, train_up=train_up, other_up=other_up, router_weight=router_weight, router_gain=router_gain)


def reference(train_gate, other_gate, train_up, other_up, router_weight, router_gain):
    latest_gate = train_gate + other_gate.astype(jnp.float32)
    latest_up = train_up + other_up.astype(jnp.float32)
    scale_gate = jnp.max(jnp.abs(latest_gate), axis=1)
    ready_gate = (latest_gate / jnp.expand_dims(scale_gate, 1)).astype(jnp.bfloat16)
    scale_up = jnp.max(jnp.abs(latest_up), axis=1)
    ready_up = (latest_up / jnp.expand_dims(scale_up, 1)).astype(jnp.bfloat16)
    serve_router = (router_weight * router_gain[:, None]).astype(jnp.bfloat16)
    return ready_gate, ready_up, scale_gate, scale_up, serve_router
```

```python
import jax
import jax.numpy as jnp
from jax import lax
from jax.experimental import pallas as pl
from jax.experimental.pallas import tpu as pltpu
from jax.sharding import PartitionSpec as P


HEAD = (1, 1)
BODY = (2, 4, 4, 3, 1)

ANY = pl.BlockSpec(memory_space=pl.ANY)
HBM = pl.BlockSpec(memory_space=pltpu.HBM)


def cost(flops, nbytes):
    return pl.CostEstimate(flops=flops, bytes_accessed=nbytes, transcendentals=0)


def latest(t, o):
    return t[0] + o[0].astype(jnp.float32)


def make(mesh):
    parts = mesh.shape["fsdp"]
    order = far_first(parts)

    def swap(x, k):
        return lax.ppermute(x, "fsdp", [(i, i ^ k) for i in range(parts)])

    def per_device(tg, og, tu, ou, router_weight, router_gain):
        experts, rows, cols = tg.shape
        width = cols // parts
        arrays = (tg, og, tu, ou)
        me = lax.axis_index("fsdp").astype(jnp.int32).reshape(1)
        smem = pl.BlockSpec(memory_space=pltpu.SMEM)

        def weights(e0):
            return [pl.BlockSpec((1, rows, cols), lambda e: (e0 + e, 0, 0))] * 4

        def peaks(e0, n, after, copies=1):
            def body(tg, og, tu, ou, *rest):
                out = rest[-1]
                e = pl.program_id(0)
                for m, (t, o) in enumerate(((tg, og), (tu, ou))):
                    top = jnp.max(jnp.abs(latest(t, o)), axis=0, keepdims=True)
                    for c in range(copies):
                        out[c, m, pl.ds(e, 1), :] = top

            return pl.pallas_call(
                body,
                grid=(n,),
                in_specs=weights(e0) + [ANY] * len(after),
                out_specs=pl.BlockSpec((copies, 2, n, cols), lambda e: (0, 0, 0, 0)),
                out_shape=jax.ShapeDtypeStruct((copies, 2, n, cols), jnp.float32),
                cost_estimate=cost(n * 3000000, n * rows * cols * 12),
                name="peaks",
            )(*arrays, *after)

        def pair_top(x, y):
            def body(me, x, y, out):
                c = me[0] & 1
                out[...] = jnp.maximum(x[c], y[c])

            return pl.pallas_call(
                body,
                in_specs=[smem] + [pl.BlockSpec(memory_space=pltpu.VMEM)] * 2,
                out_shape=jax.ShapeDtypeStruct(x.shape[1:], jnp.float32),
                name="pair_top",
            )(me, x, y)

        def all_top(xs, after):
            def body(*refs):
                top = refs[0][...]
                for r in refs[1 : len(xs)]:
                    top = jnp.maximum(top, r[...])
                refs[-1][...] = top

            return pl.pallas_call(
                body,
                in_specs=[pl.BlockSpec(memory_space=pltpu.VMEM)] * len(xs)
                + [ANY] * len(after),
                out_shape=jax.ShapeDtypeStruct(xs[0].shape, jnp.float32),
                name="all_top",
            )(*xs, *after)

        def exchange_start(peak):
            half = pair_top(peak, swap(peak, 1))
            far = [swap(half, k) for k in range(parts - 2, 0, -2)]
            return half, far

        def exchange_end(half, far, after):
            top = all_top([half] + far, after)
            return top, swap(top, 1)

        def ready(e0, n, row0, tops, after, whole=False):
            count = 1 if whole else parts
            paired = tops[0].ndim == 2

            def body(me, tg, og, tu, ou, *rest):
                outs, scale, turned = rest[-count - 2 : -2], rest[-2], rest[-1]
                e = pl.program_id(0)
                who = me[0]
                if paired:
                    even = (who & 1) == 0
                    a, b = (r[pl.ds(row0 + e, 1), :] for r in rest[:2])
                    top = (jnp.where(even, a, b), jnp.where(even, b, a))
                else:
                    top = []
                    for m in range(2):
                        t = rest[0][0, m, pl.ds(row0 + e, 1), :]
                        for d in range(1, parts):
                            t = jnp.maximum(t, rest[0][d, m, pl.ds(row0 + e, 1), :])
                        top.append(t)
                for m, (t, o) in enumerate(((tg, og), (tu, ou))):
                    scale[m, pl.ds(e, 1), :] = top[m]
                    value = (latest(t, o) / top[m]).astype(jnp.bfloat16).T
                    for d in range(parts):
                        block = value[d * width : (d + 1) * width]
                        if whole:
                            outs[0][d, m, 0] = block
                        else:
                            turned[d] = block
                    if not whole:
                        for k in range(parts):
                            outs[k][m, 0] = turned[who ^ k]

            block, shape = blocks_of(n, whole)
            small = [pl.BlockSpec(t.shape, lambda e, r=t.ndim: (0,) * r) for t in tops]
            res = pl.pallas_call(
                body,
                grid=(n,),
                in_specs=[smem] + weights(e0) + small + [ANY] * len(after),
                out_specs=[block] * count
                + [pl.BlockSpec((2, n, cols), lambda e: (0, 0, 0))],
                out_shape=[shape] * count
                + [jax.ShapeDtypeStruct((2, n, cols), jnp.float32)],
                scratch_shapes=[pltpu.VMEM((parts, width, rows), jnp.bfloat16)],
                cost_estimate=cost(n * 6000000, n * rows * cols * 16),
                name="ready",
            )(me, *arrays, *tops, *after)
            return res[:count], res[count]

        def blocks_of(n, whole):
            shape, at = (2, n, width, rows), (lambda e: (0, e, 0, 0))
            if whole:
                shape, at = (parts,) + shape, (lambda e: (0, 0, e, 0, 0))
            block = shape[:-3] + (1,) + shape[-2:]
            return pl.BlockSpec(block, at), jax.ShapeDtypeStruct(shape, jnp.bfloat16)

        def send(blocks):
            got = [blocks[0]] + [None] * (parts - 1)
            for k in order:
                got[k] = swap(blocks[k], k)
            return got

        def place(e0, n, got, full, after):
            whole = pl.BlockSpec((1, width, parts * rows), lambda e: (e0 + e, 0, 0))
            block = blocks_of(n, len(got) == 1)[0]
            shape = jax.ShapeDtypeStruct((experts, width, parts * rows), jnp.bfloat16)

            def body(me, *refs):
                ins, (gate, up) = refs[: len(got)], refs[-2:]
                for d in range(parts if len(got) == 1 else 0):
                    gate[0, :, d * rows : (d + 1) * rows] = ins[0][d, 0, 0]
                    up[0, :, d * rows : (d + 1) * rows] = ins[0][d, 1, 0]
                for k in range(parts if len(got) > 1 else 0):
                    at = pl.ds(pl.multiple_of((me[0] ^ k) * rows, rows), rows)
                    gate[0, :, at] = ins[k][0, 0]
                    up[0, :, at] = ins[k][1, 0]

            return pl.pallas_call(
                body,
                grid=(n,),
                in_specs=[smem] + [block] * len(got) + [ANY] * (len(full) + len(after)),
                out_specs=[whole, whole],
                out_shape=[shape, shape],
                input_output_aliases={1 + len(got) + i: i for i in range(len(full))},
                cost_estimate=cost(n * 3000000, n * rows * cols * 8),
                name="place",
            )(me, *got, *full, *after)

        def join(parts_of, after):
            def body(me, *refs):
                for k in range(parts):
                    at = pl.ds(pl.multiple_of((me[0] ^ k) * rows, rows), rows)
                    refs[-1][:, at] = refs[k][...]

            return pl.pallas_call(
                body,
                in_specs=[smem] + [pl.BlockSpec(memory_space=pltpu.VMEM)] * parts
                + [ANY] * len(after),
                out_shape=jax.ShapeDtypeStruct((parts_of[0].shape[0], parts * rows), jnp.bfloat16),
                name="join",
            )(me, *parts_of, *after)

        head, tail = groups(experts)
        h = sum(head)
        scales, flights = [], []

        def fly(i, e0, n, row0, tops, after):
            whole = i == 0
            blocks, scale = ready(e0, n, row0, tops, after, whole)
            scales.append(scale)
            got = [regroup(blocks[0])] if whole else send(blocks)
            flights.append((e0, n, got))
            return scale

        def regroup(x):
            return lax.all_to_all(x, "fsdp", split_axis=0, concat_axis=0, tiled=True)

        tops = (regroup(peaks(0, h, (), parts)),)
        at = fly(0, 0, head[0], 0, tops, ())
        rest = peaks(h, experts - h, (at,))
        rest = exchange_start(rest[0])
        e0 = head[0]
        for i, n in enumerate(head[1:], 1):
            at = fly(i, e0, n, e0, tops, (rest[0], at))
            e0 += n

        part_router = (router_weight * router_gain[:, None]).astype(jnp.bfloat16).T
        routers = [part_router] + [swap(part_router, k) for k in range(1, parts)]

        tops = exchange_end(*rest, (at,))
        for i, n in enumerate(tail, len(head)):
            at = fly(i, e0, n, e0 - h, tops, (at,))
            e0 += n

        scale = jnp.concatenate(scales, axis=1)
        scale = lax.dynamic_slice_in_dim(scale, lax.axis_index("fsdp") * width, width, axis=2)

        def keep(x):
            def body(x, out):
                out[...] = x[...]

            return pl.pallas_call(body, out_shape=jax.ShapeDtypeStruct(x.shape, x.dtype), name="keep")(x)

        full = ()
        for i, (e0, n, got) in enumerate(flights):
            after = ()
            if i == 2:
                serve_router = lax.all_gather(join(routers, full[:1]), "ep", axis=0, tiled=True)
                serve_router = keep(serve_router)
                after = (serve_router, scale)
            full = place(e0, n, got, full, after)
        gate, up = full
        return (
            jnp.swapaxes(gate, 1, 2),
            jnp.swapaxes(up, 1, 2),
            scale[0],
            scale[1],
            serve_router.T,
        )

    return per_device


def groups(experts):
    if sum(HEAD) + sum(BODY) == experts:
        return HEAD, BODY
    return (1, 1), (1,) * (experts - 2)


def far_first(parts):
    return [k + i for k in range(parts - 2, 0, -2) for i in (0, 1)] + [1]


def solution(mesh):
    in_specs = (P("ep", "fsdp", None),) * 4 + (P("fsdp", "ep"), P("fsdp"))
    out_specs = (P("ep", None, "fsdp"),) * 2 + (P("ep", "fsdp"),) * 2 + (P(),)
    body = make(mesh)

    def run(*args):
        mapped = jax.shard_map(
            body, mesh=mesh, in_specs=in_specs, out_specs=out_specs, check_vma=False
        )
        return mapped(*args)

    return run
```
